32 devices in a mesh: dp: 16 (over z, y, x), mp: 2 (over core).
Axes of the slice: x: 2, y: 2, z: 4, core: 2. Of those that a mesh axis runs over, the one named last changes fastest.
Arguments:
- normed: bfloat16 [6144, 2048], P(('dp', 'mp')), may hold values from -12 to 12
- key_grad: bfloat16 [6144, 512], P('dp', 'mp'), may hold values from -0.078125 to 0.078125
- stale: bfloat16 [16, 2048, 512], P('dp', None, 'mp'), may hold values from -1.5 to 1.5
- worker_flag: int32 [16], P('dp'), may hold values 0 or 1
- block_mask: int32 [16, 4], P('dp'), may hold values 0 or 1
- aggregate: float32 [2048, 512], P('dp', 'mp'), may hold values from -6 to 6
- master: float32 [2048, 512], P('dp', 'mp'), may hold values from -0.125 to 0.125
- moment_one: float32 [2048, 512], P('dp', 'mp'), may hold values from -6 to 6
- moment_two: float32 [2048, 512], P('dp', 'mp'), may hold values from 0.5 to 4
Outputs:
- new_aggregate: float32 [2048, 512], P('dp', 'mp')
- new_master: float32 [2048, 512], P('dp', 'mp')
- new_moment_one: float32 [2048, 512], P('dp', 'mp')
- new_moment_two: float32 [2048, 512], P('dp', 'mp')
- weights: bfloat16 [2048, 512], P(None, 'mp')
- new_stale: bfloat16 [16, 2048, 512], P('dp', None, 'mp')
The draws below stay inside these ranges and needn't reach their ends.
All inputs are finite; a program needn't handle non-finite values. No bound on the sum of `worker_flag` on one device may be relied on, other than what follows from the above.
Results may differ from the reference program's by a relative error of at most 0.0004.
Values may be sent and summed in bfloat16 or wider, within the bound.
A program may use at most 64 MiB of HBM per device.

```python
import math
import jax
import jax.numpy as jnp
from jax import lax

D = 2048
H = 512
BLOCKS = 4
STEP = 10
TOK_DEV = 384
TOKENS = 6144
N_DP = 16


def place_ends(values, key, least, largest):
    extent = values.shape
    index_at = [jax.random.randint(jax.random.fold_in(key, axis), (), 0, extent[axis]) for axis in range(len(extent))]
    values = values.at[tuple(index_at)].set(least)
    longest = extent.index(max(extent))
    index_at[longest] = (index_at[longest] + 1) % extent[longest]
    return values.at[tuple(index_at)].set(largest)


def with_spikes(array, own_key, source, target, blocks, factor):
    def block_of(dim):
        return (jnp.arange(array.shape[dim]) // (array.shape[dim] // blocks)).reshape((-1,) + (1,) * (array.ndim - 1 - dim))

    near = jax.random.permutation(own_key, blocks)[block_of(target)]
    far = (block_of(target) + blocks // 2) % blocks
    return jnp.where((block_of(source) == near) | (block_of(source) == far), factor * array, array)


def block_scale(rng, dims, split, smallest, high):
    level, own = 1.0, jax.random.fold_in(rng, 6)
    for dim, parts in split:
        draws = jnp.exp(jax.random.uniform(jax.random.fold_in(own, dim), (parts,), jnp.float32, smallest / len(split), high / len(split)))
        level = level * jnp.repeat(draws, dims[dim] // parts).reshape([-1 if axis == dim else 1 for axis in range(len(dims))])
    return level


def normal_values(stream_key, extent, width, bound, shards=(), held_as=jnp.bfloat16):
    loudness = block_scale(stream_key, extent, shards, -0.22, 0.18) if shards else 1.0
    drawn = jax.random.normal(stream_key, extent, jnp.float32) * width * loudness
    return jnp.minimum(jnp.maximum(drawn, -bound), bound).astype(held_as)


def bell_draw_with(rng, shape, spread, most, cuts, heavy, kind=jnp.bfloat16):
    entries = spread * jax.random.normal(rng, shape, jnp.float32)
    if cuts:
        entries = entries * block_scale(rng, shape, cuts, -0.22, 0.18)
    return jnp.clip(with_spikes(entries, jax.random.fold_in(rng, 3), *heavy), -most, most).astype(kind)


def setup_inputs(seed: int = 0) -> dict:
    streams_of = jax.random.split(jax.random.key(seed), 10)
    return {
        "normed": bell_draw_with(streams_of[0], (TOKENS, D), 1.0, 12.0, ((0, 32),), (0, 1, 32, 2.75)),
        "key_grad": normal_values(streams_of[1], (TOKENS, H), ((TOK_DEV * N_DP) ** -0.5), 0.078125, ((0, 16), (1, 2))),
        "stale": normal_values(streams_of[2], (N_DP, D, H), (N_DP ** -0.5), 1.5, ((0, 16), (2, 2))),
        "worker_flag": place_ends((jax.random.randint(streams_of[3], (N_DP,), 0, 2) < 1).astype(jnp.int32), jax.random.fold_in(streams_of[3], 1), 0, 1),
        "block_mask": place_ends((jax.random.randint(streams_of[4], (N_DP, BLOCKS), 0, 3) < 2).astype(jnp.int32), jax.random.fold_in(streams_of[4], 1), 0, 1),
        "aggregate": normal_values(streams_of[5], (D, H), 1.0, 6.0, ((0, 16), (1, 2)), jnp.float32),
        "master": normal_values(streams_of[6], (D, H), 0.02, 0.125, ((0, 16), (1, 2)), jnp.float32),
        "moment_one": normal_values(streams_of[7], (D, H), 1.0, 6.0, ((0, 16), (1, 2)), jnp.float32),
        "moment_two": jnp.clip(jnp.exp(math.log(4.0) - 2.0794415 * jax.random.uniform(streams_of[8], (D, H), jnp.float32) ** block_scale(streams_of[8], (D, H), ((0, 16), (1, 2)), -0.2, 0.2)), 0.5, 4.0),
    }


beta_one = 0.9
beta_two = 0.95
learn_rate = 0.001
decay_rate = 0.1
epsilon = 1e-08

def reference(normed, key_grad, stale, worker_flag, block_mask, aggregate, master, moment_one, moment_two):
    column_block = jnp.arange(H, dtype=jnp.int32) // (H // BLOCKS)
    onehot = (column_block[:, None] == jnp.arange(BLOCKS, dtype=jnp.int32)[None, :]).astype(jnp.int32)
    per_column = lax.optimization_barrier(jnp.sum(block_mask[:, None, :] * onehot[None, :, :], axis=2))
    trig_all = worker_flag[:, None] * per_column
    in_rows = normed.reshape(N_DP, TOK_DEV, D)
    out_rows = key_grad.reshape(N_DP, TOK_DEV, H)

    def one_worker(total, items):
        inputs, grad_out, old, trig = items
        grad = lax.dot_general(inputs, grad_out, (((0,), (0,)), ((), ())), preferred_element_type=jnp.float32)
        weight = trig.astype(jnp.float32)
        total = total + weight[None, :] * (grad - old.astype(jnp.float32))
        kept = jnp.where(trig[None, :] > 0, grad.astype(jnp.bfloat16), old)
        return (total, kept)
    summed, new_stale = lax.scan(one_worker, jnp.zeros((D, H), jnp.float32), (in_rows, out_rows, stale, trig_all))
    new_aggregate = aggregate + summed
    grads = new_aggregate
    new_moment_one = beta_one * moment_one + (1.0 - beta_one) * grads
    new_moment_two = beta_two * moment_two + (1.0 - beta_two) * grads * grads
    first_hat = new_moment_one / (1.0 - beta_one ** STEP)
    second_hat = new_moment_two / (1.0 - beta_two ** STEP)
    update = first_hat / (jnp.sqrt(second_hat) + epsilon)
    new_master = master - learn_rate * (update + decay_rate * master)
    weights = new_master.astype(jnp.bfloat16)
    return (new_aggregate, new_master, new_moment_one, new_moment_two, weights, new_stale)
```

```python
import contextlib
import functools
import math

import jax
import jax.numpy as jnp
from jax import lax
from jax.experimental import pallas as pl
from jax.experimental.pallas import tpu as pltpu
from jax.sharding import PartitionSpec as P

H = 512
BLOCKS = 4
STEP = 10


beta_one = 0.9
beta_two = 0.95
learn_rate = 0.001
decay_rate = 0.1
epsilon = 1e-08

LANES = 128
WIRE = jnp.int16
FINEST = 2.0**14
LEVELS = 1092.0
MESH = pl.DeviceIdType.MESH


def grid_of(workers):
    inner = max(i for i in range(1, math.isqrt(workers // 2) + 1) if workers % (i * i) == 0)
    return workers // (inner * inner), inner


def encode(values):
    size = jnp.log2(1.0 + jnp.abs(values) * FINEST)
    code = jnp.minimum(size * LEVELS + 0.5, 32767.0).astype(jnp.int32)
    return jnp.where(values < 0, -code, code).astype(jnp.int16)


def decode(codes):
    code = codes.astype(jnp.int32).astype(jnp.float32)
    size = (jnp.exp2(jnp.abs(code) * (1.0 / LEVELS)) - 1.0) * (1.0 / FINEST)
    return jnp.where(code < 0, -size, size)


OWN = 4
SPLIT = 1
EARLY = 8
ZORDER = (1, 2, 3)


def scope(name):
    return contextlib.nullcontext()


STEPS = (
    "W0", "C0", "x0", "C1", "R0", "d0", "X1", "C2", "X2", "C3", "X3", "V0",
    "Z0", "Z1", "Z2", "Y0", "Y1", "B0", "X4", "Y2", "Y3", "Y4",
)
GATHER = (
    "B0", "A0", "D0", "F0", "D1", "D3", "D2",
)
GATHER_OTHER = (
    "B0", "A0", "D0", "F0", "D1", "D3", "D2",
)


def early_rows(rows, ins):
    size = rows // EARLY if EARLY else 0
    return 0 if size % 16 or (ins * ins - 1) * size > rows else size


def flip(base, j, size):
    if size & (size - 1):
        return lax.rem(base + j, size)
    bit = 1
    while bit < size:
        if j & bit:
            base = base + bit - 2 * bit * lax.rem(base // bit, 2)
        bit *= 2
    return base


def kernel(
    zs, ins, mps, width,
    normed, key_grad, stale, flag, far_mask, aggregate, master, moment_one, moment_two,
    out_aggregate, out_master, out_one, out_two, full, kept,
    mine, theirs, kgrad, old, states, acc,
    part, wire, got_one, sum_one, wire_two, got_two, wire_three, own_sum, got_three,
    early, got_early, part_b, wire_b, one_b, sum_b, two_b, got_b, got_all, got_all_b,
    mask, up, down, turn, load_sem, mp_send, mp_recv, one_send, one_recv, two_send, two_recv,
    three_send, three_recv, gz_send, gz_recv, gs_send, gs_recv, gl_send, gl_recv,
    gd_send, gd_recv, early_send, early_recv, ge_send, ge_recv, gf_send, gf_recv,
):
    me = lax.axis_index("dp")
    core = lax.axis_index("mp")
    z, a, b = me // (ins * ins), lax.rem(me // ins, ins), lax.rem(me, ins)
    tokens = normed.shape[0]
    slab = normed.shape[1] // zs
    rows = slab // (ins * ins)
    cut = early_rows(rows, ins)
    late = pl.ds(cut, rows - cut)
    cols = key_grad.shape[1]

    def at(zz, aa, bb):
        return {"dp": (zz * ins + aa) * ins + bb}

    def hop(base, j, size):
        return lax.rem(base + j, size)

    loads = [
        pltpu.make_async_copy(src, dst, load_sem.at[i])
        for i, (src, dst) in enumerate(
            [(normed, mine), (key_grad, kgrad), (far_mask, mask), (stale.at[0], old)]
        )
    ]
    for load in loads:
        load.start()
    for i, src in enumerate((aggregate, master, moment_one, moment_two)):
        pltpu.make_async_copy(src, states.at[i], load_sem.at[4]).start()

    peers = [{"mp": hop(core, j, mps)} for j in range(1, mps)]
    peers += [at(z, hop(a, j, ins), b) for j in range(1, ins)]
    peers += [at(z, a, hop(b, j, ins)) for j in range(1, ins)]
    barrier = pltpu.get_barrier_semaphore()

    def signal(sem, peer):
        pl.semaphore_signal(sem, inc=1, device_id=peer, device_id_type=MESH)

    def inform(low, high, sem, step, wait):
        @pl.when((z >= low) & (z <= high))
        def _():
            if wait:
                pl.semaphore_wait(sem, 1)
            if step:
                signal(sem, at(z + step, a, b))

    for peer in peers:
        signal(barrier, peer)
    inform(1, zs - 1, barrier, -1, False)
    inform(0, zs - 2, barrier, 1, False)

    def arrive(sem, ref):
        pltpu.make_async_copy(ref, ref, sem).wait()

    def send(src, dst, send_sem, recv_sem, peer):
        copy = pltpu.make_async_remote_copy(
            src_ref=src, dst_ref=dst, send_sem=send_sem, recv_sem=recv_sem,
            device_id=peer, device_id_type=MESH,
        )
        copy.start()
        return copy

    order = list(range(zs - 1, -1, -1))

    def product(left, owner):
        held = kgrad[pl.ds(pl.multiple_of(owner * tokens, tokens), tokens), :]
        return lax.dot_general(
            left, held, (((0,), (0,)), ((), ())), preferred_element_type=jnp.float32
        )

    def columns_of(k):
        return pl.ds(pl.multiple_of(flip(z, k, zs) * slab, slab), slab)

    with scope("loads"):
        loads[0].wait()
    with scope("barrier"):
        pl.semaphore_wait(barrier, len(peers) + jnp.where(z > 0, 1, 0) + jnp.where(z < zs - 1, 1, 0))
    shared = {}
    for k in order:
        columns = columns_of(k)
        shared[k] = [
            send(
                mine.at[:, columns], theirs.at[j - 1, :, columns],
                mp_send.at[0], mp_recv.at[k, j - 1], {"mp": hop(core, j, mps)},
            )
            for j in range(1, mps)
        ]
    for j in range(1, ins):
        signal(turn, at(z, a, hop(b, j, ins)))
    inform(zs - 2, zs - 2, up, -1, False)
    inform(1, 1, down, 1, False)
    with scope("own"):
        loads[1].wait()
        for k in order[:OWN]:
            acc[columns_of(k), :] = product(mine[:, columns_of(k)], core)

    with scope("loads2"):
        for load in loads[2:4]:
            load.wait()
    block = (core * cols + lax.broadcasted_iota(jnp.int32, (1, cols), 1)) // width
    trig = jnp.zeros((1, cols), jnp.int32)
    for i in range(BLOCKS):
        trig = trig + jnp.where(block == i, flag[0] * mask[0, i], 0)
    weight = trig.astype(jnp.float32)

    def compute(k):
        columns = columns_of(k)
        grad = acc[columns, :] if k in order[:OWN] else product(mine[:, columns], core)
        for j in range(1, mps):
            with scope(f"exwait{k}"):
                shared[k][j - 1].wait_recv()
            grad = grad + product(theirs[j - 1, :, columns], hop(core, mps - j, mps))
        before = old[columns, :].astype(jnp.float32)
        kept[columns, :] = jnp.where(trig > 0, grad, before).astype(jnp.bfloat16)
        change = weight * (grad - before)
        for s in range(2):
            piece = change[:, s * LANES:(s + 1) * LANES].reshape(ins, ins, rows, LANES)
            part[s, k] = piece

    firsts, seconds, thirds = {}, {}, {}

    def group(k):
        if k == zs:
            return part_b, wire_b, one_b, sum_b, two_b, got_b, pl.ds(0, cut)
        return (part.at[:, k], wire.at[:, k], got_one.at[:, k], sum_one.at[:, k],
                wire_two.at[:, k], got_two.at[:, k], late)

    def send_early(k):
        if not cut or not k:
            return
        for s in range(2):
            early[k - 1, s] = encode(part[s, k, :, :, pl.ds(0, cut)])
        send(early.at[k - 1], got_early.at[k - 1],
             early_send.at[0], early_recv.at[k - 1], at(flip(z, k, zs), a, b))

    def sum_early(_):
        if not cut:
            return
        total = [part[s, 0, :, :, pl.ds(0, cut)] for s in range(2)]
        for k in range(zs - 1, 0, -1):
            with scope(f"we{k}"):
                arrive(early_recv.at[k - 1], got_early.at[k - 1])
            for s in range(2):
                total[s] = total[s] + decode(got_early[k - 1, s])
        for s in range(2):
            part_b[s] = total[s]

    def send_one(k):
        if k == zs and not cut:
            return
        whole, code, got, _, _, _, near = group(k)
        for j in range(1, ins):
            bb, aa = hop(b, j, ins), hop(a, j, ins)
            code[0, :, bb] = encode(whole[0, :, bb, near])
            send(code.at[0, :, bb], got.at[0, j - 1],
                 one_send.at[k], one_recv.at[k], at(z, a, bb))
            code[1, aa] = encode(whole[1, aa, :, near])
            send(code.at[1, aa], got.at[1, j - 1],
                 one_send.at[k], one_recv.at[k], at(z, aa, b))

    def send_two(k):
        if k == zs and not cut:
            return
        whole, _, got, sums, code, got_next, near = group(k)
        with scope(f"w2_{k}"):
            arrive(one_recv.at[k], got)
        for s in range(2):
            total = whole[0, :, b, near] if s == 0 else whole[1, a, :, near]
            for j in range(1, ins):
                total = total + decode(got[s, j - 1])
            sums[s] = total
            for j in range(1, ins):
                bb, aa = hop(b, j, ins), hop(a, j, ins)
                there, peer = (aa, at(z, aa, b)) if s == 0 else (bb, at(z, a, bb))
                code[s, there] = encode(sums[s, there])
                send(code.at[s, there], got_next.at[s, j - 1],
                     two_send.at[k // zs], two_recv.at[k], peer)

    def send_three(k):
        if k == zs and not cut:
            return
        _, _, _, sums, _, got, near = group(k)
        with scope(f"w3_{k}"):
            arrive(two_recv.at[k], got)
        for s in range(2):
            total = sums[s, a if s == 0 else b]
            for j in range(1, ins):
                total = total + decode(got[s, j - 1])
            if k % zs == 0:
                own_sum[s, near] = total
            else:
                wire_three[k - 1, s] = encode(total)
        if k % zs:
            send(wire_three.at[k - 1], got_three.at[k - 1],
                 three_send.at[0], three_recv.at[k - 1], at(flip(z, k, zs), a, b))

    def send_all(k, kinds=(False, True)):
        if k == zs and not cut:
            return
        whole, code, _, _, _, _, near = group(k)
        got = got_all_b if k == zs else got_all.at[:, k]
        for j in range(1, ins * ins):
            if (j // ins > 0 and j % ins > 0) not in kinds:
                continue
            aa, bb = hop(a, j // ins, ins), hop(b, j % ins, ins)
            for s in range(2):
                code[s, aa, bb] = encode(whole[s, aa, bb, near])
            send(code.at[:, aa, bb], got.at[:, j - 1],
                 one_send.at[k], one_recv.at[k], at(z, aa, bb))

    def sum_all(k):
        if k == zs and not cut:
            return
        whole, _, _, _, _, _, near = group(k)
        got = got_all_b if k == zs else got_all.at[:, k]
        with scope(f"wy_{k}"):
            arrive(one_recv.at[k], got)
        for s in range(2):
            total = whole[s, a, b, near]
            for j in range(1, ins * ins):
                total = total + decode(got[s, j - 1])
            if k % zs == 0:
                own_sum[s, near] = total
            else:
                wire_three[k - 1, s] = encode(total)
        if k % zs:
            send(wire_three.at[k - 1], got_three.at[k - 1],
                 three_send.at[0], three_recv.at[k - 1], at(flip(z, k, zs), a, b))

    def send_near(k):
        send_all(k, (False,))

    def send_diagonal(k):
        send_all(k, (True,))

    def reach_plane(_):
        pl.semaphore_wait(turn, ins - 1)

    def relay(_):
        inform(1, zs - 3, up, -1, True)
        inform(2, zs - 2, down, 1, True)

    def reach(_):
        inform(0, min(0, zs - 3), up, 0, True)
        inform(max(2, zs - 1), zs - 1, down, 0, True)

    steps = {"C": compute, "P": send_one, "T": send_two, "H": send_three, "W": relay, "V": reach, "Z": send_early, "B": sum_early, "X": send_all, "Y": sum_all, "x": send_near, "d": send_diagonal, "R": reach_plane}
    for step in STEPS:
        with scope(step):
            steps[step[0]]((order + [zs])[int(step[1])])

    arrive(load_sem.at[4], states)
    halves = [pl.ds(s * LANES, LANES) for s in range(2)]

    def update(near, last):
        for s in range(2):
            here = pl.ds(s * LANES, LANES)
            total = own_sum[s, near]
            if last:
                for k in range(1, zs):
                    total = total + decode(got_three[k - 1, s])
            new_aggregate = states[0, near, here] + total
            out_aggregate[near, here] = new_aggregate
            new_one = beta_one * states[2, near, here] + (1.0 - beta_one) * new_aggregate
            new_two = beta_two * states[3, near, here] + (1.0 - beta_two) * new_aggregate * new_aggregate
            out_one[near, here] = new_one
            out_two[near, here] = new_two
            first_hat = new_one / (1.0 - beta_one**STEP)
            second_hat = new_two / (1.0 - beta_two**STEP)
            step = first_hat / (jnp.sqrt(second_hat) + epsilon)
            held = states[1, near, here]
            new_master = held - learn_rate * (step + decay_rate * held)
            out_master[near, here] = new_master
            full[z, a, b, near, here] = new_master.astype(jnp.bfloat16)

    def update_early():
        if not cut:
            return
        near = pl.ds(0, cut)
        update(near, False)
        ref = full.at[z, a, b, near]
        for j in range(1, ins * ins):
            send(ref, ref, ge_send.at[0], ge_recv.at[0],
                 at(z, hop(a, j // ins, ins), hop(b, j % ins, ins)))

    def update_late():
        for k in order[:-1]:
            with scope(f"wz{k}"):
                arrive(three_recv.at[k - 1], got_three.at[k - 1])
        update(late, True)
        ref = full.at[z, a, b, late]
        for k in ZORDER:
            send(ref, ref, gz_send.at[0], gz_recv.at[k - 1], at(flip(z, k, zs), a, b))

    def forward():
        if not cut:
            return
        with scope("wf"):
            arrive(ge_recv.at[0], full.at[z, 0, 0, pl.ds(0, (ins * ins - 1) * cut)])
        ref = full.at[z, :, :, pl.ds(0, cut)]
        for k in range(1, zs):
            send(ref, ref, gf_send.at[0], gf_recv.at[0], at(flip(z, k, zs), a, b))

    def gather_all(k):
        ref = full.at[flip(z, k, zs), a, b, late]
        for j in range(1, ins * ins):
            send(ref, ref, gd_send.at[j - 1], gd_recv.at[j - 1],
                 at(z, hop(a, j // ins, ins), hop(b, j % ins, ins)))

    def gather_short(k):
        zz = flip(z, k, zs)
        for j in range(1, ins):
            bb, aa = hop(b, j, ins), hop(a, j, ins)
            for s, peer in ((0, at(z, aa, b)), (1, at(z, a, bb))):
                ref = full.at[zz, a, b, late, halves[s]]
                send(ref, ref, gs_send.at[0], gs_recv.at[k], peer)

    def gather_long(k):
        zz = flip(z, k, zs)
        with scope(f"wl{k}"):
            arrive(gs_recv.at[k], full.at[zz, pl.ds(0, ins - 1), 0, late])
        for j in range(1, ins):
            bb, aa = hop(b, j, ins), hop(a, j, ins)
            ref = full.at[zz, :, b, late, halves[0]]
            send(ref, ref, gl_send.at[0], gl_recv.at[0], at(z, a, bb))
            ref = full.at[zz, a, :, late, halves[1]]
            send(ref, ref, gl_send.at[0], gl_recv.at[0], at(z, aa, b))

    def blocks(n, *more):
        return full.at[pl.ds(0, n), *more, late]

    def gather(steps):
        counts = {"S": 0, "L": 0, "D": 0}
        for step in steps:
            with scope(step):
                kind, k = step[0], int(step[1])
                if kind == "A":
                    update_late()
                elif kind == "B":
                    update_early()
                elif kind == "F":
                    forward()
                else:
                    counts[kind] += 1
                    if kind == "L":
                        gather_long(k)
                    else:
                        if k:
                            with scope(f"wg{k}"):
                                arrive(gz_recv.at[k - 1], full.at[flip(z, k, zs), a, b, late])
                        (gather_all if kind == "D" else gather_short)(k)
        with scope("final"):
            if counts["L"]:
                some = blocks(counts["L"], pl.ds(0, ins - 1), pl.ds(0, ins))
                arrive(gl_recv.at[0], some)
                arrive(gs_send.at[0], blocks(counts["L"], pl.ds(0, ins - 1), 0))
                arrive(gl_send.at[0], some)
            if counts["D"]:
                for j in range(1, ins * ins):
                    arrive(gd_recv.at[j - 1], blocks(counts["D"], 0, 0))
                    arrive(gd_send.at[j - 1], blocks(counts["D"], 0, 0))

    if GATHER == GATHER_OTHER:
        gather(GATHER)
    else:
        @pl.when(core == 0)
        def _():
            gather(GATHER)

        @pl.when(core > 0)
        def _():
            gather(GATHER_OTHER)
    if cut:
        with scope("final2"):
            arrive(gf_recv.at[0], full.at[pl.ds(0, zs - 1), :, :, pl.ds(0, cut)])
    with scope("sendwait"):
        arrive(mp_send.at[0], theirs)
        for k in order:
            if f"P{order.index(k)}" in STEPS:
                arrive(one_send.at[k], got_one.at[:, k])
            else:
                arrive(one_send.at[k], got_all.at[:, k])
        halved = sum(f"P{i}" in STEPS for i in range(zs))
        if halved:
            arrive(two_send.at[0], got_two.at[:, pl.ds(zs - halved, halved)])
        arrive(three_send.at[0], got_three)
        arrive(gz_send.at[0], blocks(zs - 1, 0, 0))
        if cut:
            arrive(early_send.at[0], got_early)
            if "P4" in STEPS:
                arrive(one_send.at[zs], one_b)
                arrive(two_send.at[1], got_b)
            else:
                arrive(one_send.at[zs], got_all_b)
            arrive(ge_send.at[0], full.at[z, 0, 0, pl.ds(0, (ins * ins - 1) * cut)])
            arrive(gf_send.at[0], full.at[pl.ds(0, zs - 1), :, :, pl.ds(0, cut)])


def write_out(*refs):
    copies = []
    for src, dst in zip(refs[:6], refs[6:12]):
        parts = max(1, src.shape[0] // 512) * SPLIT
        size = src.shape[0] // parts
        for i in range(parts):
            near = pl.ds(i * size, size)
            copies.append(pltpu.make_async_copy(src.at[near], dst.at[near], refs[12].at[len(copies)]))
    with scope("wo_start"):
        for copy in reversed(copies):
            copy.start()
    with scope("wo_wait"):
        for copy in copies:
            copy.wait()


def on_device(
    workers, mps,
    normed, key_grad, stale, worker_flag, block_mask, aggregate, master, moment_one, moment_two
):
    zs, ins = grid_of(workers)
    tokens, depth = normed.shape
    cols = key_grad.shape[1]
    rows = aggregate.shape[0]
    f32, bf16 = jnp.float32, jnp.bfloat16
    dma = pltpu.SemaphoreType.DMA
    hbm = pl.BlockSpec(memory_space=pltpu.HBM)
    far = functools.partial(pltpu.with_memory_space_constraint, memory_space=pltpu.HBM)
    vmem = pl.BlockSpec(memory_space=pltpu.VMEM)
    state = jax.ShapeDtypeStruct((rows, cols), f32)
    cut = early_rows(rows, ins)
    rest, some = rows - cut, max(cut, 16)
    one = (2, zs, ins, ins, rest, LANES)
    two = (2, zs, ins, rest, LANES)
    direct = any(step[0] == "D" for step in GATHER + GATHER_OTHER)
    results = pl.pallas_call(
        functools.partial(kernel, zs, ins, mps, H // BLOCKS),
        out_shape=(
            state, state, state, state,
            jax.ShapeDtypeStruct((zs, ins, ins, rows, cols), bf16),
            jax.ShapeDtypeStruct((depth, cols), bf16),
        ),
        in_specs=[hbm] * 3 + [pl.BlockSpec(memory_space=pltpu.SMEM)] + [hbm] * 5,
        out_specs=(vmem,) * 6,
        scratch_shapes=[
            pltpu.VMEM((tokens, depth), bf16),
            pltpu.VMEM((mps - 1, tokens, depth), bf16),
            pltpu.VMEM(key_grad.shape, bf16),
            pltpu.VMEM((depth, cols), bf16),
            pltpu.VMEM((4, rows, cols), f32),
            pltpu.VMEM((depth, cols), f32),
            pltpu.VMEM((2, zs, ins, ins, rows, LANES), f32),
            pltpu.VMEM(one, WIRE),
            pltpu.VMEM((2, zs, ins - 1, ins, rest, LANES), WIRE),
            pltpu.VMEM(two, f32),
            pltpu.VMEM(two, WIRE),
            pltpu.VMEM((2, zs, ins - 1, rest, LANES), WIRE),
            pltpu.VMEM((zs - 1, 2, rest, LANES), WIRE),
            pltpu.VMEM((2, rows, LANES), f32),
            pltpu.VMEM((zs - 1, 2, rest, LANES), WIRE),
            pltpu.VMEM((zs - 1, 2, ins, ins, some, LANES), WIRE),
            pltpu.VMEM((zs - 1, 2, ins, ins, some, LANES), WIRE),
            pltpu.VMEM((2, ins, ins, some, LANES), f32),
            pltpu.VMEM((2, ins, ins, some, LANES), WIRE),
            pltpu.VMEM((2, ins - 1, ins, some, LANES), WIRE),
            pltpu.VMEM((2, ins, some, LANES), f32),
            pltpu.VMEM((2, ins, some, LANES), WIRE),
            pltpu.VMEM((2, ins - 1, some, LANES), WIRE),
            pltpu.VMEM((2, zs, ins * ins - 1, rest, LANES), WIRE),
            pltpu.VMEM((2, ins * ins - 1, some, LANES), WIRE),
            pltpu.SMEM(block_mask.shape, jnp.int32),
            pltpu.SemaphoreType.REGULAR, pltpu.SemaphoreType.REGULAR, pltpu.SemaphoreType.REGULAR,
            dma((5,)),
            dma((1,)), dma((zs, mps - 1)),
            dma((zs + 1,)), dma((zs + 1,)),
            dma((2,)), dma((zs + 1,)),
            dma((1,)), dma((zs - 1,)),
            dma((1,)), dma((zs - 1,)),
            dma((1,)), dma((zs,)),
            dma((1,)), dma((1,)),
            dma((ins * ins - 1 if direct else 1,)), dma((ins * ins - 1 if direct else 1,)),
            dma((1,)), dma((zs - 1,)),
            dma((1,)), dma((1,)), dma((1,)), dma((1,)),
        ],
        compiler_params=pltpu.CompilerParams(
            collective_id=0, has_side_effects=True, vmem_limit_bytes=48 * 1024 * 1024
        ),
    )(
        far(normed), far(key_grad), far(stale), worker_flag, far(block_mask),
        far(aggregate), far(master), far(moment_one), far(moment_two),
    )
    results = results[:4] + (results[4].reshape(depth, cols), results[5])
    results = pl.pallas_call(
        write_out,
        out_shape=tuple(pltpu.HBM(x.shape, x.dtype) for x in results),
        in_specs=[vmem] * 6,
        out_specs=(hbm,) * 6,
        scratch_shapes=[dma((4 + 2 * max(1, depth // 512) * SPLIT + 4 * SPLIT,))],
        compiler_params=pltpu.CompilerParams(vmem_limit_bytes=2 * 1024 * 1024),
    )(*results)
    return results[:5] + (results[5][None],)


def solution(mesh):
    placed = (
        P(("dp", "mp"), None),
        P("dp", "mp"),
        P("dp", None, "mp"),
        P("dp"),
        P("dp", None),
        P("dp", "mp"),
        P("dp", "mp"),
        P("dp", "mp"),
        P("dp", "mp"),
    )
    return jax.shard_map(
        functools.partial(on_device, mesh.shape["dp"], mesh.shape["mp"]),
        mesh=mesh,
        in_specs=placed,
        out_specs=(
            P("dp", "mp"),
            P("dp", "mp"),
            P("dp", "mp"),
            P("dp", "mp"),
            P(None, "mp"),
            P("dp", None, "mp"),
        ),
        check_vma=False,
    )
```

```python
import contextlib
import functools
import math

import jax
import jax.numpy as jnp
from jax import lax
from jax.experimental import pallas as pl
from jax.experimental.pallas import tpu as pltpu
from jax.sharding import PartitionSpec as P

H = 512
BLOCKS = 4
STEP = 10


beta_one = 0.9
beta_two = 0.95
learn_rate = 0.001
decay_rate = 0.1
epsilon = 1e-08

LANES = 128
WIRE = jnp.int16
FINEST = 2.0**14
LEVELS = 1092.0
MESH = pl.DeviceIdType.MESH


def grid_of(workers):
    inner = max(i for i in range(1, math.isqrt(workers // 2) + 1) if workers % (i * i) == 0)
    return workers // (inner * inner), inner


def encode(values):
    size = jnp.log2(1.0 + jnp.abs(values) * FINEST)
    code = jnp.minimum(size * LEVELS + 0.5, 32767.0).astype(jnp.int32)
    return jnp.where(values < 0, -code, code).astype(jnp.int16)


def decode(codes):
    code = codes.astype(jnp.int32).astype(jnp.float32)
    size = (jnp.exp2(jnp.abs(code) * (1.0 / LEVELS)) - 1.0) * (1.0 / FINEST)
    return jnp.where(code < 0, -size, size)


OWN = 0
SPLIT = 1
EARLY = 2
LEAD = 2
ZORDER = (1, 2, 3)


def scope(name):
    return contextlib.nullcontext()


STEPS = (
    "W0", "C0", "x0", "C1", "R0", "d0", "X1", "C2", "X2", "C3", "X3", "V0",
    "Z0", "Z1", "Z2", "Q0", "G0", "Y0", "Y1", "B0", "X4", "Y2", "Y3", "Y4",
)
STEPS_OTHER = (
    "W0", "C0", "C1", "C2", "C3", "R0", "V0", "Z0", "Z1", "Z2", "K0", "X0",
    "X1", "X2", "X3", "Y0", "Y1", "B0", "X4", "Y2", "Y3", "Y4",
)
GATHER = (
    "B0", "E0", "A0", "D0", "F0", "D1", "D3", "D2",
)
GATHER_OTHER = (
    "B0", "E0", "A0", "D0", "F0", "D1", "D3", "D2",
)


def early_rows(rows, ins, part):
    size = rows * part // 16
    return 0 if size % 8 or (ins * ins - 1) * size > rows else size


def flip(base, j, size):
    if size & (size - 1):
        return lax.rem(base + j, size)
    bit = 1
    while bit < size:
        if j & bit:
            base = base + bit - 2 * bit * lax.rem(base // bit, 2)
        bit *= 2
    return base


def kernel(
    zs, ins, mps, width,
    normed, key_grad, stale, flag, far_mask, aggregate, master, moment_one, moment_two,
    out_aggregate, out_master, out_one, out_two, full, kept,
    mine, theirs, kgrad, old, states, acc,
    part, wire, got_one, sum_one, wire_two, got_two, wire_three, own_sum, got_three,
    early, got_early, part_b, wire_b, one_b, sum_b, two_b, got_b, got_all, got_all_b,
    mask, up, down, turn, gate, load_sem, mp_send, mp_recv, one_send, one_recv, two_send, two_recv,
    three_send, three_recv, gz_send, gz_recv, gs_send, gs_recv, gl_send, gl_recv,
    gd_send, gd_recv, early_send, early_recv, ge_send, ge_recv, gf_send, gf_recv,
):
    me = lax.axis_index("dp")
    core = lax.axis_index("mp")
    z, a, b = me // (ins * ins), lax.rem(me // ins, ins), lax.rem(me, ins)
    tokens = normed.shape[0]
    slab = normed.shape[1] // zs
    rows = slab // (ins * ins)
    cut, lead = early_rows(rows, ins, EARLY), early_rows(rows, ins, LEAD)
    late, behind = pl.ds(cut, rows - cut), pl.ds(lead, rows - lead)
    cols = key_grad.shape[1]

    def at(zz, aa, bb):
        return {"dp": (zz * ins + aa) * ins + bb}

    def hop(base, j, size):
        return lax.rem(base + j, size)

    loads = [
        pltpu.make_async_copy(src, dst, load_sem.at[i])
        for i, (src, dst) in enumerate(
            [(normed, mine), (key_grad, kgrad), (far_mask, mask), (stale.at[0], old)]
        )
    ]
    for load in loads:
        load.start()
    for i, src in enumerate((aggregate, master, moment_one, moment_two)):
        pltpu.make_async_copy(src, states.at[i], load_sem.at[4]).start()

    peers = [{"mp": hop(core, j, mps)} for j in range(1, mps)]
    peers += [at(z, hop(a, j, ins), b) for j in range(1, ins)]
    peers += [at(z, a, hop(b, j, ins)) for j in range(1, ins)]
    barrier = pltpu.get_barrier_semaphore()

    def signal(sem, peer):
        pl.semaphore_signal(sem, inc=1, device_id=peer, device_id_type=MESH)

    def inform(low, high, sem, step, wait):
        @pl.when((z >= low) & (z <= high))
        def _():
            if wait:
                pl.semaphore_wait(sem, 1)
            if step:
                signal(sem, at(z + step, a, b))

    for peer in peers:
        signal(barrier, peer)
    inform(1, zs - 1, barrier, -1, False)
    inform(0, zs - 2, barrier, 1, False)

    def arrive(sem, ref):
        pltpu.make_async_copy(ref, ref, sem).wait()

    def send(src, dst, send_sem, recv_sem, peer):
        copy = pltpu.make_async_remote_copy(
            src_ref=src, dst_ref=dst, send_sem=send_sem, recv_sem=recv_sem,
            device_id=peer, device_id_type=MESH,
        )
        copy.start()
        return copy

    order = list(range(zs - 1, -1, -1))

    def product(left, owner):
        held = kgrad[pl.ds(pl.multiple_of(owner * tokens, tokens), tokens), :]
        return lax.dot_general(
            left, held, (((0,), (0,)), ((), ())), preferred_element_type=jnp.float32
        )

    def columns_of(k):
        return pl.ds(pl.multiple_of(flip(z, k, zs) * slab, slab), slab)

    with scope("loads"):
        loads[0].wait()
    with scope("own0"):
        loads[1].wait()
        for k in order[:OWN]:
            acc[columns_of(k), :] = product(mine[:, columns_of(k)], core)
    with scope("barrier"):
        pl.semaphore_wait(barrier, len(peers) + jnp.where(z > 0, 1, 0) + jnp.where(z < zs - 1, 1, 0))
    shared = {}
    for k in order:
        columns = columns_of(k)
        shared[k] = [
            send(
                mine.at[:, columns], theirs.at[j - 1, :, columns],
                mp_send.at[0], mp_recv.at[k, j - 1], {"mp": hop(core, j, mps)},
            )
            for j in range(1, mps)
        ]
    for j in range(1, ins):
        signal(turn, at(z, a, hop(b, j, ins)))
    inform(zs - 2, zs - 2, up, -1, False)
    inform(1, 1, down, 1, False)
    with scope("own"):
        for k in order[OWN:]:
            acc[columns_of(k), :] = product(mine[:, columns_of(k)], core)

    with scope("loads2"):
        for load in loads[2:4]:
            load.wait()
    block = (core * cols + lax.broadcasted_iota(jnp.int32, (1, cols), 1)) // width
    trig = jnp.zeros((1, cols), jnp.int32)
    for i in range(BLOCKS):
        trig = trig + jnp.where(block == i, flag[0] * mask[0, i], 0)
    weight = trig.astype(jnp.float32)

    def compute(k):
        columns = columns_of(k)
        grad = acc[columns, :]
        for j in range(1, mps):
            with scope(f"exwait{k}"):
                shared[k][j - 1].wait_recv()
            grad = grad + product(theirs[j - 1, :, columns], hop(core, mps - j, mps))
        before = old[columns, :].astype(jnp.float32)
        kept[columns, :] = jnp.where(trig > 0, grad, before).astype(jnp.bfloat16)
        change = weight * (grad - before)
        for s in range(2):
            piece = change[:, s * LANES:(s + 1) * LANES].reshape(ins, ins, rows, LANES)
            part[s, k] = piece

    firsts, seconds, thirds = {}, {}, {}

    def group(k):
        if k == zs:
            return part_b, wire_b, one_b, sum_b, two_b, got_b, pl.ds(0, cut)
        return (part.at[:, k], wire.at[:, k], got_one.at[:, k], sum_one.at[:, k],
                wire_two.at[:, k], got_two.at[:, k], late)

    def send_early(k):
        if not cut or not k:
            return
        for s in range(2):
            early[k - 1, s] = encode(part[s, k, :, :, pl.ds(0, cut)])
        send(early.at[k - 1], got_early.at[k - 1],
             early_send.at[0], early_recv.at[k - 1], at(flip(z, k, zs), a, b))

    def sum_early(_):
        if not cut:
            return
        total = [part[s, 0, :, :, pl.ds(0, cut)] for s in range(2)]
        for k in range(zs - 1, 0, -1):
            with scope(f"we{k}"):
                arrive(early_recv.at[k - 1], got_early.at[k - 1])
            for s in range(2):
                total[s] = total[s] + decode(got_early[k - 1, s])
        for s in range(2):
            part_b[s] = total[s]

    def send_one(k):
        if k == zs and not cut:
            return
        whole, code, got, _, _, _, near = group(k)
        for j in range(1, ins):
            bb, aa = hop(b, j, ins), hop(a, j, ins)
            code[0, :, bb] = encode(whole[0, :, bb, near])
            send(code.at[0, :, bb], got.at[0, j - 1],
                 one_send.at[k], one_recv.at[k], at(z, a, bb))
            code[1, aa] = encode(whole[1, aa, :, near])
            send(code.at[1, aa], got.at[1, j - 1],
                 one_send.at[k], one_recv.at[k], at(z, aa, b))

    def send_two(k):
        if k == zs and not cut:
            return
        whole, _, got, sums, code, got_next, near = group(k)
        with scope(f"w2_{k}"):
            arrive(one_recv.at[k], got)
        for s in range(2):
            total = whole[0, :, b, near] if s == 0 else whole[1, a, :, near]
            for j in range(1, ins):
                total = total + decode(got[s, j - 1])
            sums[s] = total
            for j in range(1, ins):
                bb, aa = hop(b, j, ins), hop(a, j, ins)
                there, peer = (aa, at(z, aa, b)) if s == 0 else (bb, at(z, a, bb))
                code[s, there] = encode(sums[s, there])
                send(code.at[s, there], got_next.at[s, j - 1],
                     two_send.at[k // zs], two_recv.at[k], peer)

    def send_three(k):
        if k == zs and not cut:
            return
        _, _, _, sums, _, got, near = group(k)
        with scope(f"w3_{k}"):
            arrive(two_recv.at[k], got)
        for s in range(2):
            total = sums[s, a if s == 0 else b]
            for j in range(1, ins):
                total = total + decode(got[s, j - 1])
            if k % zs == 0:
                own_sum[s, near] = total
            else:
                wire_three[k - 1, s] = encode(total)
        if k % zs:
            send(wire_three.at[k - 1], got_three.at[k - 1],
                 three_send.at[0], three_recv.at[k - 1], at(flip(z, k, zs), a, b))

    def send_all(k, kinds=(False, True)):
        if k == zs and not cut:
            return
        whole, code, _, _, _, _, near = group(k)
        got = got_all_b if k == zs else got_all.at[:, k]
        for j in range(1, ins * ins):
            if (j // ins > 0 and j % ins > 0) not in kinds:
                continue
            aa, bb = hop(a, j // ins, ins), hop(b, j % ins, ins)
            for s in range(2):
                code[s, aa, bb] = encode(whole[s, aa, bb, near])
            send(code.at[:, aa, bb], got.at[:, j - 1],
                 one_send.at[k], one_recv.at[k], at(z, aa, bb))

    def sum_all(k):
        if k == zs and not cut:
            return
        whole, _, _, _, _, _, near = group(k)
        got = got_all_b if k == zs else got_all.at[:, k]
        with scope(f"wy_{k}"):
            arrive(one_recv.at[k], got)
        for s in range(2):
            total = whole[s, a, b, near]
            for j in range(1, ins * ins):
                total = total + decode(got[s, j - 1])
            if k % zs == 0:
                own_sum[s, near] = total
            else:
                wire_three[k - 1, s] = encode(total)
        if k % zs:
            send(wire_three.at[k - 1], got_three.at[k - 1],
                 three_send.at[0], three_recv.at[k - 1], at(flip(z, k, zs), a, b))

    def send_near(k):
        send_all(k, (False,))

    def send_diagonal(k):
        send_all(k, (True,))

    def sent(k):
        arrive(one_send.at[k], got_all.at[:, k])

    def give(_):
        if mps > 1:
            signal(gate, {"mp": core + 1})

    def take(_):
        pl.semaphore_wait(gate, 1)

    def reach_plane(_):
        pl.semaphore_wait(turn, ins - 1)

    def relay(_):
        inform(1, zs - 3, up, -1, True)
        inform(2, zs - 2, down, 1, True)

    def reach(_):
        inform(0, min(0, zs - 3), up, 0, True)
        inform(max(2, zs - 1), zs - 1, down, 0, True)

    steps = {"C": compute, "P": send_one, "T": send_two, "H": send_three, "W": relay, "V": reach, "Z": send_early, "B": sum_early, "X": send_all, "Y": sum_all, "x": send_near, "d": send_diagonal, "R": reach_plane, "Q": sent, "G": give, "K": take}
    def reduce(names):
        for name in names:
            with scope(name):
                steps[name[0]]((order + [zs])[int(name[1])])

    def by_core(run, one, other):
        if one == other:
            return run(one)

        @pl.when(core == 0)
        def _():
            run(one)

        @pl.when(core > 0)
        def _():
            run(other)

    by_core(reduce, STEPS, STEPS_OTHER)

    arrive(load_sem.at[4], states)
    halves = [pl.ds(s * LANES, LANES) for s in range(2)]

    def update(near, last):
        for s in range(2):
            here = pl.ds(s * LANES, LANES)
            total = own_sum[s, near]
            if last:
                for k in range(1, zs):
                    total = total + decode(got_three[k - 1, s])
            new_aggregate = states[0, near, here] + total
            out_aggregate[near, here] = new_aggregate
            new_one = beta_one * states[2, near, here] + (1.0 - beta_one) * new_aggregate
            new_two = beta_two * states[3, near, here] + (1.0 - beta_two) * new_aggregate * new_aggregate
            out_one[near, here] = new_one
            out_two[near, here] = new_two
            first_hat = new_one / (1.0 - beta_one**STEP)
            second_hat = new_two / (1.0 - beta_two**STEP)
            step = first_hat / (jnp.sqrt(second_hat) + epsilon)
            held = states[1, near, here]
            new_master = held - learn_rate * (step + decay_rate * held)
            out_master[near, here] = new_master
            full[z, a, b, near, here] = new_master.astype(jnp.bfloat16)

    def update_early():
        if not cut:
            return
        update(pl.ds(0, cut), False)

    def share():
        if not lead:
            return
        ref = full.at[z, a, b, pl.ds(0, lead)]
        for j in range(1, ins * ins):
            send(ref, ref, ge_send.at[0], ge_recv.at[0],
                 at(z, hop(a, j // ins, ins), hop(b, j % ins, ins)))

    def update_late():
        for k in order[:-1]:
            with scope(f"wz{k}"):
                arrive(three_recv.at[k - 1], got_three.at[k - 1])
        update(late, True)
        ref = full.at[z, a, b, behind]
        for k in ZORDER:
            send(ref, ref, gz_send.at[0], gz_recv.at[k - 1], at(flip(z, k, zs), a, b))

    def forward():
        if not lead:
            return
        with scope("wf"):
            arrive(ge_recv.at[0], full.at[z, 0, 0, pl.ds(0, (ins * ins - 1) * lead)])
        ref = full.at[z, :, :, pl.ds(0, lead)]
        for k in range(1, zs):
            send(ref, ref, gf_send.at[0], gf_recv.at[0], at(flip(z, k, zs), a, b))

    def gather_all(k):
        ref = full.at[flip(z, k, zs), a, b, behind]
        for j in range(1, ins * ins):
            send(ref, ref, gd_send.at[j - 1], gd_recv.at[j - 1],
                 at(z, hop(a, j // ins, ins), hop(b, j % ins, ins)))

    def gather_short(k):
        zz = flip(z, k, zs)
        for j in range(1, ins):
            bb, aa = hop(b, j, ins), hop(a, j, ins)
            for s, peer in ((0, at(z, aa, b)), (1, at(z, a, bb))):
                ref = full.at[zz, a, b, behind, halves[s]]
                send(ref, ref, gs_send.at[0], gs_recv.at[k], peer)

    def gather_long(k):
        zz = flip(z, k, zs)
        with scope(f"wl{k}"):
            arrive(gs_recv.at[k], full.at[zz, pl.ds(0, ins - 1), 0, behind])
        for j in range(1, ins):
            bb, aa = hop(b, j, ins), hop(a, j, ins)
            ref = full.at[zz, :, b, behind, halves[0]]
            send(ref, ref, gl_send.at[0], gl_recv.at[0], at(z, a, bb))
            ref = full.at[zz, a, :, behind, halves[1]]
            send(ref, ref, gl_send.at[0], gl_recv.at[0], at(z, aa, b))

    def blocks(n, *more):
        return full.at[pl.ds(0, n), *more, behind]

    def gather(steps):
        counts = {"S": 0, "L": 0, "D": 0}
        for step in steps:
            with scope(step):
                kind, k = step[0], int(step[1])
                if kind == "A":
                    update_late()
                elif kind == "B":
                    update_early()
                elif kind == "E":
                    share()
                elif kind == "F":
                    forward()
                else:
                    counts[kind] += 1
                    if kind == "L":
                        gather_long(k)
                    else:
                        if k:
                            with scope(f"wg{k}"):
                                arrive(gz_recv.at[k - 1], full.at[flip(z, k, zs), a, b, behind])
                        (gather_all if kind == "D" else gather_short)(k)
        with scope("final"):
            if counts["L"]:
                some = blocks(counts["L"], pl.ds(0, ins - 1), pl.ds(0, ins))
                arrive(gl_recv.at[0], some)
                arrive(gs_send.at[0], blocks(counts["L"], pl.ds(0, ins - 1), 0))
                arrive(gl_send.at[0], some)
            if counts["D"]:
                for j in range(1, ins * ins):
                    arrive(gd_recv.at[j - 1], blocks(counts["D"], 0, 0))
                    arrive(gd_send.at[j - 1], blocks(counts["D"], 0, 0))

    by_core(gather, GATHER, GATHER_OTHER)
    if lead:
        with scope("final2"):
            arrive(gf_recv.at[0], full.at[pl.ds(0, zs - 1), :, :, pl.ds(0, lead)])
    with scope("sendwait"):
        arrive(mp_send.at[0], theirs)
        for i, k in enumerate(order):
            if f"P{i}" in STEPS:
                arrive(one_send.at[k], got_one.at[:, k])
            elif f"Q{i}" in STEPS:
                @pl.when(core > 0)
                def _(k=k):
                    arrive(one_send.at[k], got_all.at[:, k])
            else:
                arrive(one_send.at[k], got_all.at[:, k])
        halved = sum(f"P{i}" in STEPS for i in range(zs))
        if halved:
            arrive(two_send.at[0], got_two.at[:, pl.ds(zs - halved, halved)])
        arrive(three_send.at[0], got_three)
        arrive(gz_send.at[0], blocks(zs - 1, 0, 0))
        if cut:
            arrive(early_send.at[0], got_early)
            if "P4" in STEPS:
                arrive(one_send.at[zs], one_b)
                arrive(two_send.at[1], got_b)
            else:
                arrive(one_send.at[zs], got_all_b)
        if lead:
            arrive(ge_send.at[0], full.at[z, 0, 0, pl.ds(0, (ins * ins - 1) * lead)])
            arrive(gf_send.at[0], full.at[pl.ds(0, zs - 1), :, :, pl.ds(0, lead)])


def write_out(*refs):
    copies = []
    for src, dst in zip(refs[:6], refs[6:12]):
        parts = max(1, src.shape[0] // 512) * SPLIT
        size = src.shape[0] // parts
        for i in range(parts):
            near = pl.ds(i * size, size)
            copies.append(pltpu.make_async_copy(src.at[near], dst.at[near], refs[12].at[len(copies)]))
    with scope("wo_start"):
        for copy in reversed(copies):
            copy.start()
    with scope("wo_wait"):
        for copy in copies:
            copy.wait()


def on_device(
    workers, mps,
    normed, key_grad, stale, worker_flag, block_mask, aggregate, master, moment_one, moment_two
):
    zs, ins = grid_of(workers)
    tokens, depth = normed.shape
    cols = key_grad.shape[1]
    rows = aggregate.shape[0]
    f32, bf16 = jnp.float32, jnp.bfloat16
    dma = pltpu.SemaphoreType.DMA
    hbm = pl.BlockSpec(memory_space=pltpu.HBM)
    far = functools.partial(pltpu.with_memory_space_constraint, memory_space=pltpu.HBM)
    vmem = pl.BlockSpec(memory_space=pltpu.VMEM)
    state = jax.ShapeDtypeStruct((rows, cols), f32)
    cut = early_rows(rows, ins, EARLY)
    rest, some = rows - cut, max(cut, 16)
    one = (2, zs, ins, ins, rest, LANES)
    two = (2, zs, ins, rest, LANES)
    direct = any(step[0] == "D" for step in GATHER + GATHER_OTHER)
    results = pl.pallas_call(
        functools.partial(kernel, zs, ins, mps, H // BLOCKS),
        out_shape=(
            state, state, state, state,
            jax.ShapeDtypeStruct((zs, ins, ins, rows, cols), bf16),
            jax.ShapeDtypeStruct((depth, cols), bf16),
        ),
        in_specs=[hbm] * 3 + [pl.BlockSpec(memory_space=pltpu.SMEM)] + [hbm] * 5,
        out_specs=(vmem,) * 6,
        scratch_shapes=[
            pltpu.VMEM((tokens, depth), bf16),
            pltpu.VMEM((mps - 1, tokens, depth), bf16),
            pltpu.VMEM(key_grad.shape, bf16),
            pltpu.VMEM((depth, cols), bf16),
            pltpu.VMEM((4, rows, cols), f32),
            pltpu.VMEM((depth, cols), f32),
            pltpu.VMEM((2, zs, ins, ins, rows, LANES), f32),
            pltpu.VMEM(one, WIRE),
            pltpu.VMEM((2, zs, ins - 1, ins, rest, LANES), WIRE),
            pltpu.VMEM(two, f32),
            pltpu.VMEM(two, WIRE),
            pltpu.VMEM((2, zs, ins - 1, rest, LANES), WIRE),
            pltpu.VMEM((zs - 1, 2, rest, LANES), WIRE),
            pltpu.VMEM((2, rows, LANES), f32),
            pltpu.VMEM((zs - 1, 2, rest, LANES), WIRE),
            pltpu.VMEM((zs - 1, 2, ins, ins, some, LANES), WIRE),
            pltpu.VMEM((zs - 1, 2, ins, ins, some, LANES), WIRE),
            pltpu.VMEM((2, ins, ins, some, LANES), f32),
            pltpu.VMEM((2, ins, ins, some, LANES), WIRE),
            pltpu.VMEM((2, ins - 1, ins, some, LANES), WIRE),
            pltpu.VMEM((2, ins, some, LANES), f32),
            pltpu.VMEM((2, ins, some, LANES), WIRE),
            pltpu.VMEM((2, ins - 1, some, LANES), WIRE),
            pltpu.VMEM((2, zs, ins * ins - 1, rest, LANES), WIRE),
            pltpu.VMEM((2, ins * ins - 1, some, LANES), WIRE),
            pltpu.SMEM(block_mask.shape, jnp.int32),
            pltpu.SemaphoreType.REGULAR, pltpu.SemaphoreType.REGULAR, pltpu.SemaphoreType.REGULAR,
            pltpu.SemaphoreType.REGULAR,
            dma((5,)),
            dma((1,)), dma((zs, mps - 1)),
            dma((zs + 1,)), dma((zs + 1,)),
            dma((2,)), dma((zs + 1,)),
            dma((1,)), dma((zs - 1,)),
            dma((1,)), dma((zs - 1,)),
            dma((1,)), dma((zs,)),
            dma((1,)), dma((1,)),
            dma((ins * ins - 1 if direct else 1,)), dma((ins * ins - 1 if direct else 1,)),
            dma((1,)), dma((zs - 1,)),
            dma((1,)), dma((1,)), dma((1,)), dma((1,)),
        ],
        compiler_params=pltpu.CompilerParams(
            collective_id=0, has_side_effects=True, vmem_limit_bytes=48 * 1024 * 1024
        ),
    )(
        far(normed), far(key_grad), far(stale), worker_flag, far(block_mask),
        far(aggregate), far(master), far(moment_one), far(moment_two),
    )
    results = results[:4] + (results[4].reshape(depth, cols), results[5])
    results = pl.pallas_call(
        write_out,
        out_shape=tuple(pltpu.HBM(x.shape, x.dtype) for x in results),
        in_specs=[vmem] * 6,
        out_specs=(hbm,) * 6,
        scratch_shapes=[dma((4 + 2 * max(1, depth // 512) * SPLIT + 4 * SPLIT,))],
        compiler_params=pltpu.CompilerParams(vmem_limit_bytes=2 * 1024 * 1024),
    )(*results)
    return results[:5] + (results[5][None],)


def solution(mesh):
    placed = (
        P(("dp", "mp"), None),
        P("dp", "mp"),
        P("dp", None, "mp"),
        P("dp"),
        P("dp", None),
        P("dp", "mp"),
        P("dp", "mp"),
        P("dp", "mp"),
        P("dp", "mp"),
    )
    return jax.shard_map(
        functools.partial(on_device, mesh.shape["dp"], mesh.shape["mp"]),
        mesh=mesh,
        in_specs=placed,
        out_specs=(
            P("dp", "mp"),
            P("dp", "mp"),
            P("dp", "mp"),
            P("dp", "mp"),
            P(None, "mp"),
            P("dp", None, "mp"),
        ),
        check_vma=False,
    )
```

```python
import contextlib
import functools
import math

import jax
import jax.numpy as jnp
from jax import lax
from jax.experimental import pallas as pl
from jax.experimental.pallas import tpu as pltpu
from jax.sharding import PartitionSpec as P

H = 512
BLOCKS = 4
STEP = 10


beta_one = 0.9
beta_two = 0.95
learn_rate = 0.001
decay_rate = 0.1
epsilon = 1e-08

LANES = 128
WIRE = jnp.int16
FINEST = 2.0**14
LEVELS = 1092.0
MESH = pl.DeviceIdType.MESH


def grid_of(workers):
    inner = max(i for i in range(1, math.isqrt(workers // 2) + 1) if workers % (i * i) == 0)
    return workers // (inner * inner), inner


def encode(values):
    size = jnp.log2(1.0 + jnp.abs(values) * FINEST)
    code = jnp.minimum(size * LEVELS + 0.5, 32767.0).astype(jnp.int32)
    return jnp.where(values < 0, -code, code).astype(jnp.int16)


def decode(codes):
    code = codes.astype(jnp.int32).astype(jnp.float32)
    size = (jnp.exp2(jnp.abs(code) * (1.0 / LEVELS)) - 1.0) * (1.0 / FINEST)
    return jnp.where(code < 0, -size, size)


OWN = 0
EARLY = 2
LEAD = 4
ZORDER = (1, 2, 3)


def scope(name):
    return contextlib.nullcontext()


STEPS = (
    "W0", "C0", "x0", "C1", "R0", "d0", "X1", "C2", "X2", "C3", "X3", "Z2",
    "V0", "Z0", "Z1", "Q0", "G0", "Y0", "Y1", "B0", "X4", "Y2", "Y3", "Y4",
)
STEPS_OTHER = (
    "W0", "C0", "C1", "C2", "C3", "R0", "V0", "K0", "X0", "X1", "X2", "X3",
    "Z0", "Z1", "Z2", "Y0", "Y1", "B0", "X4", "Y2", "Y3", "Y4",
)
GATHER = (
    "B0", "A0", "E0", "D0", "D1", "F0", "D3", "D2",
)
GATHER_OTHER = (
    "B0", "A0", "E0", "D0", "D1", "F0", "D3", "D2",
)


def early_rows(rows, ins, part):
    size = rows * part // 16
    return 0 if size % 8 or (ins * ins - 1) * size > rows else size


def flip(base, j, size):
    if size & (size - 1):
        return lax.rem(base + j, size)
    bit = 1
    while bit < size:
        if j & bit:
            base = base + bit - 2 * bit * lax.rem(base // bit, 2)
        bit *= 2
    return base


def kernel(
    zs, ins, mps, width,
    normed, key_grad, stale, flag, far_mask, aggregate, master, moment_one, moment_two,
    out_aggregate, out_master, out_one, out_two, full, kept,
    mine, theirs, kgrad, old, states, acc,
    part, wire, got_all, wire_three, own_sum, got_three,
    early, got_early, part_b, wire_b, got_all_b,
    mask, up, down, turn, gate, load_sem, mp_send, mp_recv, one_send, one_recv,
    three_send, three_recv, gz_send, gz_recv, gd_send, gd_recv, early_send, early_recv, ge_send, ge_recv, gf_send, gf_recv,
):
    me = lax.axis_index("dp")
    core = lax.axis_index("mp")
    z, a, b = me // (ins * ins), lax.rem(me // ins, ins), lax.rem(me, ins)
    tokens = normed.shape[0]
    slab = normed.shape[1] // zs
    rows = slab // (ins * ins)
    cut, lead = early_rows(rows, ins, EARLY), early_rows(rows, ins, LEAD)
    late, behind = pl.ds(cut, rows - cut), pl.ds(lead, rows - lead)
    cols = key_grad.shape[1]

    def at(zz, aa, bb):
        return {"dp": (zz * ins + aa) * ins + bb}

    def hop(base, j, size):
        return lax.rem(base + j, size)

    loads = [
        pltpu.make_async_copy(src, dst, load_sem.at[i])
        for i, (src, dst) in enumerate(
            [(normed, mine), (key_grad, kgrad), (far_mask, mask), (stale.at[0], old)]
        )
    ]
    for load in loads:
        load.start()
    for i, src in enumerate((aggregate, master, moment_one, moment_two)):
        pltpu.make_async_copy(src, states.at[i], load_sem.at[4]).start()

    peers = [{"mp": hop(core, j, mps)} for j in range(1, mps)]
    peers += [at(z, hop(a, j, ins), b) for j in range(1, ins)]
    peers += [at(z, a, hop(b, j, ins)) for j in range(1, ins)]
    barrier = pltpu.get_barrier_semaphore()

    def signal(sem, peer):
        pl.semaphore_signal(sem, inc=1, device_id=peer, device_id_type=MESH)

    def inform(low, high, sem, step, wait):
        @pl.when((z >= low) & (z <= high))
        def _():
            if wait:
                pl.semaphore_wait(sem, 1)
            if step:
                signal(sem, at(z + step, a, b))

    for peer in peers:
        signal(barrier, peer)
    inform(1, zs - 1, barrier, -1, False)
    inform(0, zs - 2, barrier, 1, False)

    def arrive(sem, ref):
        pltpu.make_async_copy(ref, ref, sem).wait()

    def send(src, dst, send_sem, recv_sem, peer):
        copy = pltpu.make_async_remote_copy(
            src_ref=src, dst_ref=dst, send_sem=send_sem, recv_sem=recv_sem,
            device_id=peer, device_id_type=MESH,
        )
        copy.start()
        return copy

    order = list(range(zs - 1, -1, -1))

    def product(left, owner):
        held = kgrad[pl.ds(pl.multiple_of(owner * tokens, tokens), tokens), :]
        return lax.dot_general(
            left, held, (((0,), (0,)), ((), ())), preferred_element_type=jnp.float32
        )

    def columns_of(k):
        return pl.ds(pl.multiple_of(flip(z, k, zs) * slab, slab), slab)

    with scope("loads"):
        loads[0].wait()
    with scope("own0"):
        loads[1].wait()
        for k in order[:OWN]:
            acc[columns_of(k), :] = product(mine[:, columns_of(k)], core)
    with scope("barrier"):
        pl.semaphore_wait(barrier, len(peers) + jnp.where(z > 0, 1, 0) + jnp.where(z < zs - 1, 1, 0))
    shared = {}
    for k in order:
        columns = columns_of(k)
        shared[k] = [
            send(
                mine.at[:, columns], theirs.at[j - 1, :, columns],
                mp_send.at[0], mp_recv.at[k, j - 1], {"mp": hop(core, j, mps)},
            )
            for j in range(1, mps)
        ]
    for j in range(1, ins):
        signal(turn, at(z, a, hop(b, j, ins)))
    inform(zs - 2, zs - 2, up, -1, False)
    inform(1, 1, down, 1, False)
    with scope("own"):
        for k in order[OWN:]:
            acc[columns_of(k), :] = product(mine[:, columns_of(k)], core)

    with scope("loads2"):
        for load in loads[2:4]:
            load.wait()
    block = (core * cols + lax.broadcasted_iota(jnp.int32, (1, cols), 1)) // width
    trig = jnp.zeros((1, cols), jnp.int32)
    for i in range(BLOCKS):
        trig = trig + jnp.where(block == i, flag[0] * mask[0, i], 0)
    weight = trig.astype(jnp.float32)

    def compute(k):
        columns = columns_of(k)
        grad = acc[columns, :]
        for j in range(1, mps):
            with scope(f"exwait{k}"):
                shared[k][j - 1].wait_recv()
            grad = grad + product(theirs[j - 1, :, columns], hop(core, mps - j, mps))
        before = old[columns, :].astype(jnp.float32)
        kept[columns, :] = jnp.where(trig > 0, grad, before).astype(jnp.bfloat16)
        change = weight * (grad - before)
        for s in range(2):
            piece = change[:, s * LANES:(s + 1) * LANES].reshape(ins, ins, rows, LANES)
            part[s, k] = piece

    firsts, seconds, thirds = {}, {}, {}

    def group(k):
        if k == zs:
            return part_b, wire_b, got_all_b, pl.ds(0, cut)
        return part.at[:, k], wire.at[:, k], got_all.at[:, k], late

    def send_early(k):
        if not cut or not k:
            return
        for s in range(2):
            early[k - 1, s] = encode(part[s, k, :, :, pl.ds(0, cut)])
        send(early.at[k - 1], got_early.at[k - 1],
             early_send.at[0], early_recv.at[k - 1], at(flip(z, k, zs), a, b))

    def sum_early(_):
        if not cut:
            return
        total = [part[s, 0, :, :, pl.ds(0, cut)] for s in range(2)]
        for k in range(zs - 1, 0, -1):
            with scope(f"we{k}"):
                arrive(early_recv.at[k - 1], got_early.at[k - 1])
            for s in range(2):
                total[s] = total[s] + decode(got_early[k - 1, s])
        for s in range(2):
            part_b[s] = total[s]

    def send_all(k, kinds=(False, True)):
        if k == zs and not cut:
            return
        whole, code, got, near = group(k)
        for j in range(1, ins * ins):
            if (j // ins > 0 and j % ins > 0) not in kinds:
                continue
            aa, bb = hop(a, j // ins, ins), hop(b, j % ins, ins)
            for s in range(2):
                code[s, aa, bb] = encode(whole[s, aa, bb, near])
            send(code.at[:, aa, bb], got.at[:, j - 1],
                 one_send.at[k], one_recv.at[k], at(z, aa, bb))

    def sum_all(k):
        if k == zs and not cut:
            return
        whole, _, got, near = group(k)
        with scope(f"wy_{k}"):
            arrive(one_recv.at[k], got)
        for s in range(2):
            total = whole[s, a, b, near]
            for j in range(1, ins * ins):
                total = total + decode(got[s, j - 1])
            if k % zs == 0:
                own_sum[s, near] = total
            else:
                wire_three[k - 1, s] = encode(total)
        if k % zs:
            send(wire_three.at[k - 1], got_three.at[k - 1],
                 three_send.at[0], three_recv.at[k - 1], at(flip(z, k, zs), a, b))

    def send_near(k):
        send_all(k, (False,))

    def send_diagonal(k):
        send_all(k, (True,))

    def sent(k):
        arrive(one_send.at[k], got_all.at[:, k])

    def give(_):
        if mps > 1:
            signal(gate, {"mp": core + 1})

    def take(_):
        pl.semaphore_wait(gate, 1)

    def reach_plane(_):
        pl.semaphore_wait(turn, ins - 1)

    def relay(_):
        inform(1, zs - 3, up, -1, True)
        inform(2, zs - 2, down, 1, True)

    def reach(_):
        inform(0, min(0, zs - 3), up, 0, True)
        inform(max(2, zs - 1), zs - 1, down, 0, True)

    steps = {"C": compute, "W": relay, "V": reach, "Z": send_early, "B": sum_early, "X": send_all, "Y": sum_all, "x": send_near, "d": send_diagonal, "R": reach_plane, "Q": sent, "G": give, "K": take}
    def reduce(names):
        for name in names:
            with scope(name):
                steps[name[0]]((order + [zs])[int(name[1])])

    def by_core(run, one, other):
        if one == other:
            return run(one)

        @pl.when(core == 0)
        def _():
            run(one)

        @pl.when(core > 0)
        def _():
            run(other)

    def drain(names):
        for i, k in enumerate(order):
            if f"Q{i}" not in names:
                sent(k)
        if cut:
            arrive(one_send.at[zs], got_all_b)

    by_core(reduce, STEPS, STEPS_OTHER)

    arrive(load_sem.at[4], states)

    def update(near, last):
        for s in range(2):
            here = pl.ds(s * LANES, LANES)
            total = own_sum[s, near]
            if last:
                for k in range(1, zs):
                    total = total + decode(got_three[k - 1, s])
            new_aggregate = states[0, near, here] + total
            out_aggregate[near, here] = new_aggregate
            new_one = beta_one * states[2, near, here] + (1.0 - beta_one) * new_aggregate
            new_two = beta_two * states[3, near, here] + (1.0 - beta_two) * new_aggregate * new_aggregate
            out_one[near, here] = new_one
            out_two[near, here] = new_two
            first_hat = new_one / (1.0 - beta_one**STEP)
            second_hat = new_two / (1.0 - beta_two**STEP)
            step = first_hat / (jnp.sqrt(second_hat) + epsilon)
            held = states[1, near, here]
            new_master = held - learn_rate * (step + decay_rate * held)
            out_master[near, here] = new_master
            full[z, a, b, near, here] = new_master.astype(jnp.bfloat16)

    def update_early():
        if not cut:
            return
        update(pl.ds(0, cut), False)

    def share():
        if not lead:
            return
        ref = full.at[z, a, b, pl.ds(0, lead)]
        for j in range(1, ins * ins):
            send(ref, ref, ge_send.at[0], ge_recv.at[0],
                 at(z, hop(a, j // ins, ins), hop(b, j % ins, ins)))

    def update_late():
        for k in order[:-1]:
            with scope(f"wz{k}"):
                arrive(three_recv.at[k - 1], got_three.at[k - 1])
        update(late, True)
        ref = full.at[z, a, b, behind]
        for k in ZORDER:
            send(ref, ref, gz_send.at[0], gz_recv.at[k - 1], at(flip(z, k, zs), a, b))

    def forward():
        if not lead:
            return
        with scope("wf"):
            arrive(ge_recv.at[0], full.at[z, 0, 0, pl.ds(0, (ins * ins - 1) * lead)])
        ref = full.at[z, :, :, pl.ds(0, lead)]
        for k in range(1, zs):
            send(ref, ref, gf_send.at[0], gf_recv.at[0], at(flip(z, k, zs), a, b))

    def gather_all(k):
        if k:
            with scope(f"wg{k}"):
                arrive(gz_recv.at[k - 1], full.at[flip(z, k, zs), a, b, behind])
        ref = full.at[flip(z, k, zs), a, b, behind]
        for j in range(1, ins * ins):
            send(ref, ref, gd_send.at[j - 1], gd_recv.at[j - 1],
                 at(z, hop(a, j // ins, ins), hop(b, j % ins, ins)))

    actions = {"A": update_late, "B": update_early, "E": share, "F": forward}

    def gather(names):
        for name in names:
            with scope(name):
                if name[0] == "D":
                    gather_all(int(name[1]))
                else:
                    actions[name[0]]()

    by_core(gather, GATHER, GATHER_OTHER)
    with scope("final"):
        for j in range(1, ins * ins):
            arrive(gd_recv.at[j - 1], full.at[:, 0, 0, behind])
    if lead:
        with scope("final2"):
            arrive(gf_recv.at[0], full.at[pl.ds(0, zs - 1), :, :, pl.ds(0, lead)])
    with scope("sendwait"):
        for j in range(1, ins * ins):
            arrive(gd_send.at[j - 1], full.at[:, 0, 0, behind])
        arrive(mp_send.at[0], theirs)
        by_core(drain, STEPS, STEPS_OTHER)
        arrive(three_send.at[0], got_three)
        arrive(gz_send.at[0], full.at[pl.ds(0, zs - 1), 0, 0, behind])
        if cut:
            arrive(early_send.at[0], got_early)
        if lead:
            arrive(ge_send.at[0], full.at[z, 0, 0, pl.ds(0, (ins * ins - 1) * lead)])
            arrive(gf_send.at[0], full.at[pl.ds(0, zs - 1), :, :, pl.ds(0, lead)])


def write_out(*refs):
    copies = [
        pltpu.make_async_copy(src, dst, refs[12].at[i])
        for i, (src, dst) in enumerate(zip(refs[:6], refs[6:12]))
    ]
    with scope("wo_start"):
        for copy in reversed(copies):
            copy.start()
    with scope("wo_wait"):
        for copy in copies:
            copy.wait()


def on_device(
    workers, mps,
    normed, key_grad, stale, worker_flag, block_mask, aggregate, master, moment_one, moment_two
):
    zs, ins = grid_of(workers)
    tokens, depth = normed.shape
    cols = key_grad.shape[1]
    rows = aggregate.shape[0]
    f32, bf16 = jnp.float32, jnp.bfloat16
    dma = pltpu.SemaphoreType.DMA
    hbm = pl.BlockSpec(memory_space=pltpu.HBM)
    far = functools.partial(pltpu.with_memory_space_constraint, memory_space=pltpu.HBM)
    vmem = pl.BlockSpec(memory_space=pltpu.VMEM)
    state = jax.ShapeDtypeStruct((rows, cols), f32)
    cut = early_rows(rows, ins, EARLY)
    rest, some = rows - cut, max(cut, 16)
    results = pl.pallas_call(
        functools.partial(kernel, zs, ins, mps, H // BLOCKS),
        out_shape=(
            state, state, state, state,
            jax.ShapeDtypeStruct((zs, ins, ins, rows, cols), bf16),
            jax.ShapeDtypeStruct((depth, cols), bf16),
        ),
        in_specs=[hbm] * 3 + [pl.BlockSpec(memory_space=pltpu.SMEM)] + [hbm] * 5,
        out_specs=(vmem,) * 6,
        scratch_shapes=[
            pltpu.VMEM((tokens, depth), bf16),
            pltpu.VMEM((mps - 1, tokens, depth), bf16),
            pltpu.VMEM(key_grad.shape, bf16),
            pltpu.VMEM((depth, cols), bf16),
            pltpu.VMEM((4, rows, cols), f32),
            pltpu.VMEM((depth, cols), f32),
            pltpu.VMEM((2, zs, ins, ins, rows, LANES), f32),
            pltpu.VMEM((2, zs, ins, ins, rest, LANES), WIRE),
            pltpu.VMEM((2, zs, ins * ins - 1, rest, LANES), WIRE),
            pltpu.VMEM((zs - 1, 2, rest, LANES), WIRE),
            pltpu.VMEM((2, rows, LANES), f32),
            pltpu.VMEM((zs - 1, 2, rest, LANES), WIRE),
            pltpu.VMEM((zs - 1, 2, ins, ins, some, LANES), WIRE),
            pltpu.VMEM((zs - 1, 2, ins, ins, some, LANES), WIRE),
            pltpu.VMEM((2, ins, ins, some, LANES), f32),
            pltpu.VMEM((2, ins, ins, some, LANES), WIRE),
            pltpu.VMEM((2, ins * ins - 1, some, LANES), WIRE),
            pltpu.SMEM(block_mask.shape, jnp.int32),
            pltpu.SemaphoreType.REGULAR, pltpu.SemaphoreType.REGULAR, pltpu.SemaphoreType.REGULAR,
            pltpu.SemaphoreType.REGULAR,
            dma((5,)),
            dma((1,)), dma((zs, mps - 1)),
            dma((zs + 1,)), dma((zs + 1,)),
            dma((1,)), dma((zs - 1,)),
            dma((1,)), dma((zs - 1,)),
            dma((ins * ins - 1,)), dma((ins * ins - 1,)),
            dma((1,)), dma((zs - 1,)),
            dma((1,)), dma((1,)), dma((1,)), dma((1,)),
        ],
        compiler_params=pltpu.CompilerParams(
            collective_id=0, has_side_effects=True, vmem_limit_bytes=48 * 1024 * 1024
        ),
    )(
        far(normed), far(key_grad), far(stale), worker_flag, far(block_mask),
        far(aggregate), far(master), far(moment_one), far(moment_two),
    )
    results = results[:4] + (results[4].reshape(depth, cols), results[5])
    results = pl.pallas_call(
        write_out,
        out_shape=tuple(pltpu.HBM(x.shape, x.dtype) for x in results),
        in_specs=[vmem] * 6,
        out_specs=(hbm,) * 6,
        scratch_shapes=[dma((6,))],
        compiler_params=pltpu.CompilerParams(vmem_limit_bytes=2 * 1024 * 1024),
    )(*results)
    return results[:5] + (results[5][None],)


def solution(mesh):
    placed = (
        P(("dp", "mp"), None),
        P("dp", "mp"),
        P("dp", None, "mp"),
        P("dp"),
        P("dp", None),
        P("dp", "mp"),
        P("dp", "mp"),
        P("dp", "mp"),
        P("dp", "mp"),
    )
    return jax.shard_map(
        functools.partial(on_device, mesh.shape["dp"], mesh.shape["mp"]),
        mesh=mesh,
        in_specs=placed,
        out_specs=(
            P("dp", "mp"),
            P("dp", "mp"),
            P("dp", "mp"),
            P("dp", "mp"),
            P(None, "mp"),
            P("dp", None, "mp"),
        ),
        check_vma=False,
    )
```

```python
import contextlib
import functools
import math

import jax
import jax.numpy as jnp
from jax import lax
from jax.experimental import pallas as pl
from jax.experimental.pallas import tpu as pltpu
from jax.sharding import PartitionSpec as P

H = 512
BLOCKS = 4
STEP = 10


beta_one = 0.9
beta_two = 0.95
learn_rate = 0.001
decay_rate = 0.1
epsilon = 1e-08

LANES = 128
WIRE = jnp.int16
FINEST = 2.0**14
LEVELS = 1092.0
MESH = pl.DeviceIdType.MESH


def grid_of(workers):
    inner = max(i for i in range(1, math.isqrt(workers // 2) + 1) if workers % (i * i) == 0)
    return workers // (inner * inner), inner


def encode(values):
    size = jnp.log2(1.0 + jnp.abs(values) * FINEST)
    code = jnp.minimum(size * LEVELS + 0.5, 32767.0).astype(jnp.int32)
    return jnp.where(values < 0, -code, code).astype(jnp.int16)


def decode(codes):
    code = codes.astype(jnp.int32).astype(jnp.float32)
    size = (jnp.exp2(jnp.abs(code) * (1.0 / LEVELS)) - 1.0) * (1.0 / FINEST)
    return jnp.where(code < 0, -size, size)


OWN = 0
EARLY = 2
LEAD = 4
HALVED = True


def scope(name):
    return contextlib.nullcontext()


STEPS = (
    "W0", "C0", "x0", "C1", "R0", "d0", "X1", "C2", "X2", "C3", "X3", "Z2",
    "V0", "Z0", "Z1", "Q0", "G0", "Y0", "Y1", "B0", "X4", "Y2", "Y3", "Y4",
)
STEPS_OTHER = (
    "W0", "C0", "C1", "C2", "C3", "R0", "V0", "K0", "X0", "Z0", "X1", "Z1",
    "X2", "Z2", "X3", "Y0", "Y1", "B0", "X4", "Y2", "Y3", "Y4",
)
GATHER = (
    "B0", "A0", "E0", "D0", "D1", "F0", "D3", "D2",
)
GATHER_OTHER = (
    "B0", "A0", "E0", "D0", "D1", "F0", "D3", "D2",
)


def early_rows(rows, ins, part):
    size = rows * part // 16
    return 0 if size % 8 or (ins * ins - 1) * size > rows else size


def flip(base, j, size):
    if size & (size - 1):
        return lax.rem(base + j, size)
    bit = 1
    while bit < size:
        if j & bit:
            base = base + bit - 2 * bit * lax.rem(base // bit, 2)
        bit *= 2
    return base


def kernel(
    zs, ins, mps, width,
    normed, key_grad, stale, flag, far_mask, aggregate, master, moment_one, moment_two,
    out_aggregate, out_master, out_one, out_two, full, kept,
    mine, theirs, kgrad, old, states, acc,
    part, wire, got_all, wire_three, own_sum, got_three,
    early, got_early, part_b, wire_b, got_all_b,
    mask, up, down, turn, gate, load_sem, mp_send, mp_recv, one_send, one_recv,
    three_send, three_recv, gz_send, gz_recv, gd_send, gd_recv, early_send, early_recv, ge_send, ge_recv, gf_send, gf_recv,
):
    me = lax.axis_index("dp")
    core = lax.axis_index("mp")
    z, a, b = me // (ins * ins), lax.rem(me // ins, ins), lax.rem(me, ins)
    tokens = normed.shape[0]
    slab = normed.shape[1] // zs
    rows = slab // (ins * ins)
    cut, lead = early_rows(rows, ins, EARLY), early_rows(rows, ins, LEAD)
    late, behind = pl.ds(cut, rows - cut), pl.ds(lead, rows - lead)
    half = (rows - lead) // 2
    edges = [lead, lead + half, rows] if HALVED and half % 8 == 0 else [lead, rows]
    parts = [pl.ds(low, high - low) for low, high in zip(edges, edges[1:])]
    cols = key_grad.shape[1]

    def at(zz, aa, bb):
        return {"dp": (zz * ins + aa) * ins + bb}

    def hop(base, j, size):
        return lax.rem(base + j, size)

    loads = [
        pltpu.make_async_copy(src, dst, load_sem.at[i])
        for i, (src, dst) in enumerate(
            [(normed, mine), (key_grad, kgrad), (far_mask, mask), (stale.at[0], old)]
        )
    ]
    for load in loads:
        load.start()
    for i, src in enumerate((aggregate, master, moment_one, moment_two)):
        pltpu.make_async_copy(src, states.at[i], load_sem.at[4]).start()

    peers = [{"mp": hop(core, j, mps)} for j in range(1, mps)]
    peers += [at(z, hop(a, j, ins), b) for j in range(1, ins)]
    peers += [at(z, a, hop(b, j, ins)) for j in range(1, ins)]
    barrier = pltpu.get_barrier_semaphore()

    def signal(sem, peer):
        pl.semaphore_signal(sem, inc=1, device_id=peer, device_id_type=MESH)

    def inform(low, high, sem, step, wait):
        @pl.when((z >= low) & (z <= high))
        def _():
            if wait:
                pl.semaphore_wait(sem, 1)
            if step:
                signal(sem, at(z + step, a, b))

    for peer in peers:
        signal(barrier, peer)
    inform(1, zs - 1, barrier, -1, False)
    inform(0, zs - 2, barrier, 1, False)

    def arrive(sem, ref):
        pltpu.make_async_copy(ref, ref, sem).wait()

    def send(src, dst, send_sem, recv_sem, peer):
        copy = pltpu.make_async_remote_copy(
            src_ref=src, dst_ref=dst, send_sem=send_sem, recv_sem=recv_sem,
            device_id=peer, device_id_type=MESH,
        )
        copy.start()
        return copy

    order = list(range(zs - 1, -1, -1))

    def product(left, owner):
        held = kgrad[pl.ds(pl.multiple_of(owner * tokens, tokens), tokens), :]
        return lax.dot_general(
            left, held, (((0,), (0,)), ((), ())), preferred_element_type=jnp.float32
        )

    def columns_of(k):
        return pl.ds(pl.multiple_of(flip(z, k, zs) * slab, slab), slab)

    with scope("loads"):
        loads[0].wait()
    with scope("own0"):
        loads[1].wait()
        for k in order[:OWN]:
            acc[columns_of(k), :] = product(mine[:, columns_of(k)], core)
    with scope("barrier"):
        pl.semaphore_wait(barrier, len(peers) + jnp.where(z > 0, 1, 0) + jnp.where(z < zs - 1, 1, 0))
    shared = {}
    for k in order:
        columns = columns_of(k)
        shared[k] = [
            send(
                mine.at[:, columns], theirs.at[j - 1, :, columns],
                mp_send.at[0], mp_recv.at[k, j - 1], {"mp": hop(core, j, mps)},
            )
            for j in range(1, mps)
        ]
    for j in range(1, ins):
        signal(turn, at(z, a, hop(b, j, ins)))
    inform(zs - 2, zs - 2, up, -1, False)
    inform(1, 1, down, 1, False)
    with scope("own"):
        for k in order[OWN:]:
            acc[columns_of(k), :] = product(mine[:, columns_of(k)], core)

    with scope("loads2"):
        for load in loads[2:4]:
            load.wait()
    block = (core * cols + lax.broadcasted_iota(jnp.int32, (1, cols), 1)) // width
    trig = jnp.zeros((1, cols), jnp.int32)
    for i in range(BLOCKS):
        trig = trig + jnp.where(block == i, flag[0] * mask[0, i], 0)
    weight = trig.astype(jnp.float32)

    def compute(k):
        columns = columns_of(k)
        grad = acc[columns, :]
        for j in range(1, mps):
            with scope(f"exwait{k}"):
                shared[k][j - 1].wait_recv()
            grad = grad + product(theirs[j - 1, :, columns], hop(core, mps - j, mps))
        before = old[columns, :].astype(jnp.float32)
        kept[columns, :] = jnp.where(trig > 0, grad, before).astype(jnp.bfloat16)
        change = weight * (grad - before)
        for s in range(2):
            piece = change[:, s * LANES:(s + 1) * LANES].reshape(ins, ins, rows, LANES)
            part[s, k] = piece

    firsts, seconds, thirds = {}, {}, {}

    def group(k):
        if k == zs:
            return part_b, wire_b, got_all_b, pl.ds(0, cut)
        return part.at[:, k], wire.at[:, k], got_all.at[:, k], late

    def send_early(k):
        if not cut or not k:
            return
        for s in range(2):
            early[k - 1, s] = encode(part[s, k, :, :, pl.ds(0, cut)])
        send(early.at[k - 1], got_early.at[k - 1],
             early_send.at[0], early_recv.at[k - 1], at(flip(z, k, zs), a, b))

    def sum_early(_):
        if not cut:
            return
        total = [part[s, 0, :, :, pl.ds(0, cut)] for s in range(2)]
        for k in range(zs - 1, 0, -1):
            with scope(f"we{k}"):
                arrive(early_recv.at[k - 1], got_early.at[k - 1])
            for s in range(2):
                total[s] = total[s] + decode(got_early[k - 1, s])
        for s in range(2):
            part_b[s] = total[s]

    def send_all(k, kinds=(False, True)):
        if k == zs and not cut:
            return
        whole, code, got, near = group(k)
        for j in range(1, ins * ins):
            if (j // ins > 0 and j % ins > 0) not in kinds:
                continue
            aa, bb = hop(a, j // ins, ins), hop(b, j % ins, ins)
            for s in range(2):
                code[s, aa, bb] = encode(whole[s, aa, bb, near])
            send(code.at[:, aa, bb], got.at[:, j - 1],
                 one_send.at[k], one_recv.at[k], at(z, aa, bb))

    def sum_all(k):
        if k == zs and not cut:
            return
        whole, _, got, near = group(k)
        with scope(f"wy_{k}"):
            arrive(one_recv.at[k], got)
        for s in range(2):
            total = whole[s, a, b, near]
            for j in range(1, ins * ins):
                total = total + decode(got[s, j - 1])
            if k % zs == 0:
                own_sum[s, near] = total
            else:
                wire_three[k - 1, s] = encode(total)
        if k % zs:
            send(wire_three.at[k - 1], got_three.at[k - 1],
                 three_send.at[0], three_recv.at[k - 1], at(flip(z, k, zs), a, b))

    def send_near(k):
        send_all(k, (False,))

    def send_diagonal(k):
        send_all(k, (True,))

    def sent(k):
        arrive(one_send.at[k], got_all.at[:, k])

    def give(_):
        if mps > 1:
            signal(gate, {"mp": core + 1})

    def take(_):
        pl.semaphore_wait(gate, 1)

    def reach_plane(_):
        pl.semaphore_wait(turn, ins - 1)

    def relay(_):
        inform(1, zs - 3, up, -1, True)
        inform(2, zs - 2, down, 1, True)

    def reach(_):
        inform(0, min(0, zs - 3), up, 0, True)
        inform(max(2, zs - 1), zs - 1, down, 0, True)

    steps = {"C": compute, "W": relay, "V": reach, "Z": send_early, "B": sum_early, "X": send_all, "Y": sum_all, "x": send_near, "d": send_diagonal, "R": reach_plane, "Q": sent, "G": give, "K": take}
    def reduce(names):
        for name in names:
            with scope(name):
                steps[name[0]]((order + [zs])[int(name[1])])

    def by_core(run, one, other):
        if one == other:
            return run(one)

        @pl.when(core == 0)
        def _():
            run(one)

        @pl.when(core > 0)
        def _():
            run(other)

    def drain(names):
        for i, k in enumerate(order):
            if f"Q{i}" not in names:
                sent(k)
        if cut:
            arrive(one_send.at[zs], got_all_b)

    by_core(reduce, STEPS, STEPS_OTHER)

    arrive(load_sem.at[4], states)

    def update(low, high, last):
        near, there = pl.ds(low, high - low), pl.ds(low - cut, high - low)
        for s in range(2):
            here = pl.ds(s * LANES, LANES)
            total = own_sum[s, near]
            if last:
                for k in range(1, zs):
                    total = total + decode(got_three[k - 1, s, there])
            new_aggregate = states[0, near, here] + total
            out_aggregate[near, here] = new_aggregate
            new_one = beta_one * states[2, near, here] + (1.0 - beta_one) * new_aggregate
            new_two = beta_two * states[3, near, here] + (1.0 - beta_two) * new_aggregate * new_aggregate
            out_one[near, here] = new_one
            out_two[near, here] = new_two
            first_hat = new_one / (1.0 - beta_one**STEP)
            second_hat = new_two / (1.0 - beta_two**STEP)
            step = first_hat / (jnp.sqrt(second_hat) + epsilon)
            held = states[1, near, here]
            new_master = held - learn_rate * (step + decay_rate * held)
            out_master[near, here] = new_master
            full[z, a, b, near, here] = new_master.astype(jnp.bfloat16)

    def update_early():
        if not cut:
            return
        update(0, cut, False)

    def share():
        if not lead:
            return
        ref = full.at[z, a, b, pl.ds(0, lead)]
        for j in range(1, ins * ins):
            send(ref, ref, ge_send.at[0], ge_recv.at[0],
                 at(z, hop(a, j // ins, ins), hop(b, j % ins, ins)))

    def update_late(turns):
        for k in order[:-1]:
            with scope(f"wz{k}"):
                arrive(three_recv.at[k - 1], got_three.at[k - 1])
        low = cut
        for h, high in enumerate(edges[1:]):
            update(low, high, True)
            low = high
            ref = full.at[z, a, b, parts[h]]
            for k in turns:
                send(ref, ref, gz_send.at[0], gz_recv.at[k - 1, h], at(flip(z, k, zs), a, b))

    def forward():
        if not lead:
            return
        with scope("wf"):
            arrive(ge_recv.at[0], full.at[z, 0, 0, pl.ds(0, (ins * ins - 1) * lead)])
        ref = full.at[z, :, :, pl.ds(0, lead)]
        for k in range(1, zs):
            send(ref, ref, gf_send.at[0], gf_recv.at[0], at(flip(z, k, zs), a, b))

    def gather_all(k):
        for h, part_rows in enumerate(parts):
            ref = full.at[flip(z, k, zs), a, b, part_rows]
            if k:
                with scope(f"wg{k}{h}"):
                    arrive(gz_recv.at[k - 1, h], ref)
            for j in range(1, ins * ins):
                send(ref, ref, gd_send.at[j - 1], gd_recv.at[j - 1],
                     at(z, hop(a, j // ins, ins), hop(b, j % ins, ins)))

    actions = {"B": update_early, "E": share, "F": forward}

    def gather(names):
        for name in names:
            with scope(name):
                if name[0] == "D":
                    gather_all(int(name[1]))
                elif name[0] == "A":
                    update_late([k for k in range(1, zs)][:: -1 if name == "A1" else 1])
                else:
                    actions[name[0]]()

    by_core(gather, GATHER, GATHER_OTHER)
    with scope("final"):
        for j in range(1, ins * ins):
            arrive(gd_recv.at[j - 1], full.at[:, 0, 0, behind])
    if lead:
        with scope("final2"):
            arrive(gf_recv.at[0], full.at[pl.ds(0, zs - 1), :, :, pl.ds(0, lead)])
    with scope("sendwait"):
        for j in range(1, ins * ins):
            arrive(gd_send.at[j - 1], full.at[:, 0, 0, behind])
        arrive(mp_send.at[0], theirs)
        by_core(drain, STEPS, STEPS_OTHER)
        arrive(three_send.at[0], got_three)
        arrive(gz_send.at[0], full.at[pl.ds(0, zs - 1), 0, 0, behind])
        if cut:
            arrive(early_send.at[0], got_early)
        if lead:
            arrive(ge_send.at[0], full.at[z, 0, 0, pl.ds(0, (ins * ins - 1) * lead)])
            arrive(gf_send.at[0], full.at[pl.ds(0, zs - 1), :, :, pl.ds(0, lead)])


def write_out(*refs):
    copies = [
        pltpu.make_async_copy(src, dst, refs[12].at[i])
        for i, (src, dst) in enumerate(zip(refs[:6], refs[6:12]))
    ]
    with scope("wo_start"):
        for copy in reversed(copies):
            copy.start()
    with scope("wo_wait"):
        for copy in copies:
            copy.wait()


def on_device(
    workers, mps,
    normed, key_grad, stale, worker_flag, block_mask, aggregate, master, moment_one, moment_two
):
    zs, ins = grid_of(workers)
    tokens, depth = normed.shape
    cols = key_grad.shape[1]
    rows = aggregate.shape[0]
    f32, bf16 = jnp.float32, jnp.bfloat16
    dma = pltpu.SemaphoreType.DMA
    hbm = pl.BlockSpec(memory_space=pltpu.HBM)
    far = functools.partial(pltpu.with_memory_space_constraint, memory_space=pltpu.HBM)
    vmem = pl.BlockSpec(memory_space=pltpu.VMEM)
    state = jax.ShapeDtypeStruct((rows, cols), f32)
    cut = early_rows(rows, ins, EARLY)
    rest, some = rows - cut, max(cut, 16)
    results = pl.pallas_call(
        functools.partial(kernel, zs, ins, mps, H // BLOCKS),
        out_shape=(
            state, state, state, state,
            jax.ShapeDtypeStruct((zs, ins, ins, rows, cols), bf16),
            jax.ShapeDtypeStruct((depth, cols), bf16),
        ),
        in_specs=[hbm] * 3 + [pl.BlockSpec(memory_space=pltpu.SMEM)] + [hbm] * 5,
        out_specs=(vmem,) * 6,
        scratch_shapes=[
            pltpu.VMEM((tokens, depth), bf16),
            pltpu.VMEM((mps - 1, tokens, depth), bf16),
            pltpu.VMEM(key_grad.shape, bf16),
            pltpu.VMEM((depth, cols), bf16),
            pltpu.VMEM((4, rows, cols), f32),
            pltpu.VMEM((depth, cols), f32),
            pltpu.VMEM((2, zs, ins, ins, rows, LANES), f32),
            pltpu.VMEM((2, zs, ins, ins, rest, LANES), WIRE),
            pltpu.VMEM((2, zs, ins * ins - 1, rest, LANES), WIRE),
            pltpu.VMEM((zs - 1, 2, rest, LANES), WIRE),
            pltpu.VMEM((2, rows, LANES), f32),
            pltpu.VMEM((zs - 1, 2, rest, LANES), WIRE),
            pltpu.VMEM((zs - 1, 2, ins, ins, some, LANES), WIRE),
            pltpu.VMEM((zs - 1, 2, ins, ins, some, LANES), WIRE),
            pltpu.VMEM((2, ins, ins, some, LANES), f32),
            pltpu.VMEM((2, ins, ins, some, LANES), WIRE),
            pltpu.VMEM((2, ins * ins - 1, some, LANES), WIRE),
            pltpu.SMEM(block_mask.shape, jnp.int32),
            pltpu.SemaphoreType.REGULAR, pltpu.SemaphoreType.REGULAR, pltpu.SemaphoreType.REGULAR,
            pltpu.SemaphoreType.REGULAR,
            dma((5,)),
            dma((1,)), dma((zs, mps - 1)),
            dma((zs + 1,)), dma((zs + 1,)),
            dma((1,)), dma((zs - 1,)),
            dma((1,)), dma((zs - 1, 2)),
            dma((ins * ins - 1,)), dma((ins * ins - 1,)),
            dma((1,)), dma((zs - 1,)),
            dma((1,)), dma((1,)), dma((1,)), dma((1,)),
        ],
        compiler_params=pltpu.CompilerParams(
            collective_id=0, has_side_effects=True, vmem_limit_bytes=48 * 1024 * 1024
        ),
    )(
        far(normed), far(key_grad), far(stale), worker_flag, far(block_mask),
        far(aggregate), far(master), far(moment_one), far(moment_two),
    )
    results = results[:4] + (results[4].reshape(depth, cols), results[5])
    results = pl.pallas_call(
        write_out,
        out_shape=tuple(pltpu.HBM(x.shape, x.dtype) for x in results),
        in_specs=[vmem] * 6,
        out_specs=(hbm,) * 6,
        scratch_shapes=[dma((6,))],
        compiler_params=pltpu.CompilerParams(vmem_limit_bytes=2 * 1024 * 1024),
    )(*results)
    return results[:5] + (results[5][None],)


def solution(mesh):
    placed = (
        P(("dp", "mp"), None),
        P("dp", "mp"),
        P("dp", None, "mp"),
        P("dp"),
        P("dp", None),
        P("dp", "mp"),
        P("dp", "mp"),
        P("dp", "mp"),
        P("dp", "mp"),
    )
    return jax.shard_map(
        functools.partial(on_device, mesh.shape["dp"], mesh.shape["mp"]),
        mesh=mesh,
        in_specs=placed,
        out_specs=(
            P("dp", "mp"),
            P("dp", "mp"),
            P("dp", "mp"),
            P("dp", "mp"),
            P(None, "mp"),
            P("dp", None, "mp"),
        ),
        check_vma=False,
    )
```
